32 devices in a mesh: dp: 4 (over y, z), tp: 8 (over x, core).
Axes of the slice: x: 4, y: 2, z: 2, core: 2. Of those that a mesh axis runs over, the one named last changes fastest.
The devices are a block of a 4x4x8 slice.
Arguments:
- mel_in: bfloat16 [8, 4096, 80], P('dp', 'tp'), parts along dimension 0
- pos_table: float32 [2048, 512], P('tp')
- w_conv1: bfloat16 [3, 80, 512], replicated
- b_conv1: bfloat16 [512], replicated
- w_conv2: bfloat16 [3, 512, 512], replicated
- b_conv2: bfloat16 [512], replicated
- ln1_gain: bfloat16 [512], replicated
- ln1_bias: bfloat16 [512], replicated
- w_query: bfloat16 [512, 512], P(None, 'tp')
- b_query: bfloat16 [512], P('tp')
- w_key: bfloat16 [512, 512], P(None, 'tp')
- w_value: bfloat16 [512, 512], P(None, 'tp')
- b_value: bfloat16 [512], P('tp')
- w_out: bfloat16 [512, 512], P('tp')
- b_out: bfloat16 [512], replicated
- ln2_gain: bfloat16 [512], replicated
- ln2_bias: bfloat16 [512], replicated
- w_fc1: bfloat16 [512, 2048], P(None, 'tp')
- b_fc1: bfloat16 [2048], P('tp')
- w_fc2: bfloat16 [2048, 512], P('tp')
- b_fc2: bfloat16 [512], replicated
- grad_y: bfloat16 [8, 2048, 512], P('dp', 'tp'), parts along dimension 0
Outputs:
- output 1: bfloat16 [8, 2048, 512], P('dp', 'tp'), parts along dimension 0
- output 2: bfloat16 [8, 4096, 80], P('dp', 'tp'), parts along dimension 0
- output 3: float32 [12, 80, 512], P('dp'), parts along dimension 0
- output 4: float32 [2048], P('dp'), parts along dimension 0
- output 5: float32 [12, 512, 512], P('dp'), parts along dimension 0
- output 6: float32 [2048], P('dp'), parts along dimension 0
- output 7: float32 [2048], P('dp'), parts along dimension 0
- output 8: float32 [2048], P('dp'), parts along dimension 0
- output 9: float32 [2048, 512], P('dp', 'tp'), parts along dimension 0
- output 10: float32 [2048], P(('dp', 'tp')), parts along dimension 0
- output 11: float32 [2048, 512], P('dp', 'tp'), parts along dimension 0
- output 12: float32 [2048, 512], P('dp', 'tp'), parts along dimension 0
- output 13: float32 [2048], P(('dp', 'tp')), parts along dimension 0
- output 14: float32 [2048, 512], P(('dp', 'tp')), parts along dimension 0
- output 15: float32 [2048], P('dp'), parts along dimension 0
- output 16: float32 [2048], P('dp'), parts along dimension 0
- output 17: float32 [2048], P('dp'), parts along dimension 0
- output 18: float32 [2048, 2048], P('dp', 'tp'), parts along dimension 0
- output 19: float32 [8192], P(('dp', 'tp')), parts along dimension 0
- output 20: float32 [8192, 512], P(('dp', 'tp')), parts along dimension 0
- output 21: float32 [2048], P('dp'), parts along dimension 0
There are 4 independent parts. The reference program is written for one: setup_inputs(seed, part) draws one part's arguments, and reference() takes and returns one part's arrays. A program takes and returns all parts, laid end to end along the dimension named above; an argument that names none is the same for every part.
All inputs are finite; a program needn't handle non-finite values.
Results may differ from the reference program's by a relative error of at most 0.02.
Values are sent between devices in bfloat16 or wider.
A program may use at most 768 MiB of HBM per device.

```python
import jax
import jax.numpy as jnp
from jax import lax

BATCH = 2
FRAMES = 2048
D = 512
HEADS = 8
MEL = 80
HEAD_DIM = 64
LN_EPS = 1e-5
SCORE_SCALE = HEAD_DIM ** -0.5


def draw_normal(rng_key, array_shape, factor):
    return (jax.random.normal(rng_key, array_shape, jnp.float32) * factor).astype(jnp.bfloat16)


def draw_gain(rng_key):
    return (1.0 + 0.3 * jax.random.normal(rng_key, (D,), jnp.float32)).astype(jnp.bfloat16)


def setup_inputs(seed: int = 0, part: int = 0) -> dict:
    base_key = jax.random.key(seed)
    key_list = jax.random.split(base_key, 20)
    own_keys = jax.random.split(jax.random.fold_in(base_key, part), 2)
    hidden_width = 4 * D
    return {
        'mel_in': draw_normal(own_keys[0], (BATCH, 2 * FRAMES, MEL), 1.0),
        'pos_table': jax.random.normal(key_list[0], (FRAMES, D), jnp.float32) * 0.7,
        'w_conv1': draw_normal(key_list[1], (3, MEL, D), (3 * MEL) ** -0.5),
        'b_conv1': draw_normal(key_list[2], (D,), 0.5),
        'w_conv2': draw_normal(key_list[3], (3, D, D), (3 * D) ** -0.5),
        'b_conv2': draw_normal(key_list[4], (D,), 0.5),
        'ln1_gain': draw_gain(key_list[5]),
        'ln1_bias': draw_normal(key_list[6], (D,), 0.3),
        'w_query': draw_normal(key_list[7], (D, D), 1.4 * D ** -0.5),
        'b_query': draw_normal(key_list[8], (D,), 0.5),
        'w_key': draw_normal(key_list[9], (D, D), 1.4 * D ** -0.5),
        'w_value': draw_normal(key_list[10], (D, D), D ** -0.5),
        'b_value': draw_normal(key_list[11], (D,), 0.3),
        'w_out': draw_normal(key_list[12], (D, D), 2.0 * D ** -0.5),
        'b_out': draw_normal(key_list[13], (D,), 0.3),
        'ln2_gain': draw_gain(key_list[14]),
        'ln2_bias': draw_normal(key_list[15], (D,), 0.3),
        'w_fc1': draw_normal(key_list[16], (D, hidden_width), D ** -0.5),
        'b_fc1': draw_normal(key_list[17], (hidden_width,), 0.5),
        'w_fc2': draw_normal(key_list[18], (hidden_width, D), hidden_width ** -0.5),
        'b_fc2': draw_normal(key_list[19], (D,), 0.3),
        'grad_y': draw_normal(own_keys[1], (BATCH, FRAMES, D), 1.0),
    }


def gelu_exact(values):
    return jax.nn.gelu(values, approximate=False)


def flat_dot(lhs, rhs):
    lead_dims = lhs.shape[:-1]
    result = jnp.dot(lhs.reshape(-1, lhs.shape[-1]), rhs, preferred_element_type=jnp.float32)
    return result.reshape(lead_dims + (rhs.shape[-1],))


def layer_norm(values, gain_vec, shift_vec):
    x_f32 = values.astype(jnp.float32)
    row_mean = jnp.mean(x_f32, axis=-1, keepdims=True)
    centred = x_f32 - row_mean
    row_var = jnp.mean(centred * centred, axis=-1, keepdims=True)
    normed = centred * lax.rsqrt(row_var + LN_EPS) * gain_vec.astype(jnp.float32) + shift_vec.astype(jnp.float32)
    return normed.astype(jnp.bfloat16)


def encoder_forward(mel_in, pos_table, weights):
    (w_conv1, b_conv1, w_conv2, b_conv2, ln1_gain, ln1_bias, w_query, b_query, w_key, w_value,
     b_value, w_out, b_out, ln2_gain, ln2_bias, w_fc1, b_fc1, w_fc2, b_fc2) = weights
    n_batch, mel_len, n_mel = mel_in.shape
    frames = mel_len // 2
    model_width = w_conv2.shape[-1]
    mel_pad = jnp.pad(mel_in, ((0, 0), (1, 1), (0, 0)))
    windows = jnp.stack([mel_pad[:, tap_idx:tap_idx + mel_len] for tap_idx in range(3)], axis=2)
    h1_pre = flat_dot(windows.reshape(n_batch, mel_len, 3 * n_mel), w_conv1.reshape(3 * n_mel, model_width)) + b_conv1.astype(jnp.float32)
    h1_pad = jnp.pad(gelu_exact(h1_pre).astype(jnp.bfloat16), ((0, 0), (1, 1), (0, 0)))
    h1_pairs = h1_pad[:, :mel_len].reshape(n_batch, frames, 2 * model_width)
    h1_after = h1_pad[:, 2:].reshape(n_batch, frames, 2, model_width)[:, :, 0]
    h2_pre = (flat_dot(h1_pairs, w_conv2[:2].reshape(2 * model_width, model_width))
              + flat_dot(h1_after, w_conv2[2]) + b_conv2.astype(jnp.float32))
    x_embed = (gelu_exact(h2_pre) + pos_table).astype(jnp.bfloat16)
    norm_one = layer_norm(x_embed, ln1_gain, ln1_bias)
    head_shape = (n_batch, frames, HEADS, HEAD_DIM)
    q_heads = (flat_dot(norm_one, w_query) + b_query.astype(jnp.float32)).astype(jnp.bfloat16).reshape(head_shape)
    k_heads = flat_dot(norm_one, w_key).astype(jnp.bfloat16).reshape(head_shape)
    v_heads = (flat_dot(norm_one, w_value) + b_value.astype(jnp.float32)).astype(jnp.bfloat16).reshape(head_shape)
    scores = jnp.einsum('bqhe,bkhe->bhqk', q_heads.astype(jnp.float32), k_heads.astype(jnp.float32)) * SCORE_SCALE
    attn_probs = jax.nn.softmax(scores, axis=-1).astype(jnp.bfloat16)
    attn_heads = jnp.einsum('bhqk,bkhe->bqhe', attn_probs.astype(jnp.float32), v_heads.astype(jnp.float32))
    attn_flat = attn_heads.astype(jnp.bfloat16).reshape(n_batch, frames, model_width)
    x_mid = (x_embed.astype(jnp.float32) + flat_dot(attn_flat, w_out) + b_out.astype(jnp.float32)).astype(jnp.bfloat16)
    norm_two = layer_norm(x_mid, ln2_gain, ln2_bias)
    hidden = gelu_exact(flat_dot(norm_two, w_fc1) + b_fc1.astype(jnp.float32)).astype(jnp.bfloat16)
    return (x_mid.astype(jnp.float32) + flat_dot(hidden, w_fc2) + b_fc2.astype(jnp.float32)).astype(jnp.bfloat16)


def reference(mel_in, pos_table, w_conv1, b_conv1, w_conv2, b_conv2, ln1_gain, ln1_bias, w_query, b_query,
              w_key, w_value, b_value, w_out, b_out, ln2_gain, ln2_bias, w_fc1, b_fc1, w_fc2, b_fc2, grad_y):
    weights = (w_conv1, b_conv1, w_conv2, b_conv2, ln1_gain, ln1_bias, w_query, b_query, w_key, w_value,
               b_value, w_out, b_out, ln2_gain, ln2_bias, w_fc1, b_fc1, w_fc2, b_fc2)

    def forward_part(mel_arg, weight_arg):
        return encoder_forward(mel_arg, pos_table, weight_arg)

    y_out, pullback = jax.vjp(forward_part, mel_in, weights)
    d_mel, d_weights = pullback(grad_y)
    (g_conv1_w, g_conv1_b, g_conv2_w, g_conv2_b, g_ln1_gain, g_ln1_bias, g_query_w, g_query_b, g_key_w,
     g_value_w, g_value_b, g_out_w, g_out_b, g_ln2_gain, g_ln2_bias, g_fc1_w, g_fc1_b, g_fc2_w,
     g_fc2_b) = [grad_w.astype(jnp.float32) for grad_w in d_weights]
    return (y_out, d_mel, g_conv1_w, g_conv1_b, g_conv2_w, g_conv2_b, g_ln1_gain, g_ln1_bias, g_query_w,
            g_query_b, g_key_w, g_value_w, g_value_b, g_out_w, g_out_b, g_ln2_gain, g_ln2_bias, g_fc1_w,
            g_fc1_b, g_fc2_w, g_fc2_b)
```

```python
import functools
import math
import jax
import jax.numpy as jnp
from jax import lax
from jax.experimental import pallas as pl
from jax.experimental.pallas import tpu as pltpu
from jax.sharding import PartitionSpec as P

HEAD_DIM = 64
LN_EPS = 1e-5
BF = jnp.bfloat16
F32 = jnp.float32
LANES = 128
BIAS_ROWS = 16
VEC_ROWS = 8


def dims(lhs, rhs, contract_lhs, contract_rhs):
    return lax.dot_general(lhs, rhs, (((contract_lhs,), (contract_rhs,)), ((), ())), preferred_element_type=F32)


def mm(lhs, rhs):
    return dims(lhs, rhs, 1, 0)


def mm_nt(lhs, rhs):
    return dims(lhs, rhs, 1, 1)


def mm_tn(lhs, rhs):
    return dims(lhs, rhs, 0, 0)


def phi_cdf(x):
    return 0.5 * (1.0 + lax.erf(x * (0.5 ** 0.5)))


def gelu(x):
    return x * phi_cdf(x)


def gelu_grad(x):
    return phi_cdf(x) + x * (jnp.exp(x * x * -0.5) * (1.0 / math.sqrt(2.0 * math.pi)))


def norm_stats(x):
    centred = x - jnp.mean(x, axis=-1, keepdims=True)
    rstd = lax.rsqrt(jnp.mean(centred * centred, axis=-1, keepdims=True) + LN_EPS)
    return centred * rstd, rstd


def norm_back(d_out, x_hat, rstd, gain):
    a = d_out * gain
    return rstd * (a - jnp.mean(a, axis=-1, keepdims=True) - x_hat * jnp.mean(a * x_hat, axis=-1, keepdims=True))


def colsum(x):
    return jnp.sum(x, axis=0, keepdims=True)


def peer(index):
    return {'tp': index}


def entry_barrier(size, me):
    barrier = pltpu.get_barrier_semaphore()
    for step in range(1, size):
        pl.semaphore_signal(barrier, inc=1, device_id=peer(lax.rem(me + step, size)), device_id_type=pl.DeviceIdType.MESH)
    pl.semaphore_wait(barrier, size - 1)


def exchange_kernel(size, x_ref, out_ref, send_sem, recv_sem, own_sem):
    me = lax.axis_index('tp')
    entry_barrier(size, me)
    copies = []
    for step in range(1, size):
        to = lax.rem(me + step, size)
        copies.append(pltpu.make_async_remote_copy(
            src_ref=x_ref.at[to], dst_ref=out_ref.at[me], send_sem=send_sem.at[step], recv_sem=recv_sem.at[step],
            device_id=peer(to), device_id_type=pl.DeviceIdType.MESH))
        copies[-1].start()
    own = pltpu.make_async_copy(x_ref.at[me], out_ref.at[me], own_sem)
    own.start()
    own.wait()
    for copy in copies:
        copy.wait()


def exchange(x, size, cid):
    return pl.pallas_call(
        functools.partial(exchange_kernel, size),
        out_shape=jax.ShapeDtypeStruct(x.shape, x.dtype),
        in_specs=[pl.BlockSpec(memory_space=pltpu.VMEM)],
        out_specs=pl.BlockSpec(memory_space=pl.ANY),
        scratch_shapes=[pltpu.SemaphoreType.DMA((size,)), pltpu.SemaphoreType.DMA((size,)), pltpu.SemaphoreType.DMA],
        compiler_params=pltpu.CompilerParams(collective_id=cid, has_side_effects=True),
        name=f'exchange{cid}',
    )(x)


def all_sum_kernel(size, x_ref, out_ref, parts, mine, whole, send_a, recv_a, send_b, recv_b):
    me = lax.axis_index('tp')
    entry_barrier(size, me)
    copies = []
    for step in range(1, size):
        to = lax.rem(me + step, size)
        copies.append(pltpu.make_async_remote_copy(
            src_ref=x_ref.at[to], dst_ref=parts.at[step], send_sem=send_a.at[step], recv_sem=recv_a.at[step],
            device_id=peer(to), device_id_type=pl.DeviceIdType.MESH))
        copies[-1].start()
    for copy in copies:
        copy.wait()
    total = x_ref[me].astype(F32)
    for step in range(1, size):
        total = total + parts[step].astype(F32)
    mine[...] = total.astype(BF)
    copies = []
    for step in range(1, size):
        to = lax.rem(me + step, size)
        copies.append(pltpu.make_async_remote_copy(
            src_ref=mine, dst_ref=whole.at[me], send_sem=send_b.at[step], recv_sem=recv_b.at[step],
            device_id=peer(to), device_id_type=pl.DeviceIdType.MESH))
        copies[-1].start()
    for copy in copies:
        copy.wait()
    out_ref[...] = whole[...].astype(F32)
    out_ref[me] = mine[...].astype(F32)


def all_sum(x, size, cid):
    return pl.pallas_call(
        functools.partial(all_sum_kernel, size),
        out_shape=jax.ShapeDtypeStruct(x.shape, F32),
        in_specs=[pl.BlockSpec(memory_space=pltpu.VMEM)],
        out_specs=pl.BlockSpec(memory_space=pltpu.VMEM),
        scratch_shapes=[pltpu.VMEM(x.shape, BF), pltpu.VMEM(x.shape[1:], BF), pltpu.VMEM(x.shape, BF)]
        + [pltpu.SemaphoreType.DMA((size,))] * 4,
        compiler_params=pltpu.CompilerParams(collective_id=cid, has_side_effects=True),
        name=f'all_sum{cid}',
    )(x)


def load_mel(m_scr, mel_ref, halo_ref):
    mel_len, n_mel = mel_ref.shape[1:]
    total = m_scr.shape[0]
    m_scr[0:8, :] = jnp.zeros((8, m_scr.shape[1]), F32)
    m_scr[8 + mel_len:total, :] = jnp.zeros((total - 8 - mel_len, m_scr.shape[1]), F32)
    m_scr[8:8 + mel_len, 0:n_mel] = mel_ref[0].astype(F32)
    halo = halo_ref[0].astype(F32)
    m_scr[6:8, 0:n_mel] = halo[0:2]
    m_scr[8 + mel_len:10 + mel_len, 0:n_mel] = halo[2:4]


def mel_taps(m_scr, rows, n_mel):
    return [m_scr[pl.ds(5 + tap, rows, stride=2), :].astype(BF)[:, 0:n_mel] for tap in range(4)]


def conv_one(taps, w_ref, bias):
    even = mm(taps[0], w_ref[0]) + mm(taps[1], w_ref[1]) + mm(taps[2], w_ref[2]) + bias
    odd = mm(taps[1], w_ref[0]) + mm(taps[2], w_ref[1]) + mm(taps[3], w_ref[2]) + bias
    return even, odd


def row_ids(rows, width):
    return lax.broadcasted_iota(jnp.int32, (rows, width), 0)


def front_kernel(mel_ref, halo_ref, pos_ref, w1_ref, w2_ref, vec_ref, h1_ref, h2_ref, x_ref, n1_ref, m_scr, e_scr, o_scr):
    rank = lax.axis_index('tp')
    n_mel = mel_ref.shape[2]
    frames, width = pos_ref.shape
    rows = e_scr.shape[0]
    load_mel(m_scr, mel_ref, halo_ref)
    even, odd = conv_one(mel_taps(m_scr, rows, n_mel), w1_ref, vec_ref[0:1, :])
    e_scr[...] = gelu(even)
    o_scr[...] = gelu(odd)

    @pl.when(rank == 0)
    def _():
        o_scr[0:1, :] = jnp.zeros((1, width), F32)

    h1_ref[0, :, 0:width] = o_scr[0:frames, :].astype(BF)
    h1_ref[0, :, width:2 * width] = e_scr[1:frames + 1, :].astype(BF)
    h1_ref[0, :, 2 * width:3 * width] = o_scr[1:frames + 1, :].astype(BF)
    h2_pre = mm(h1_ref[0], w2_ref[...]) + vec_ref[1:2, :]
    h2_ref[0] = h2_pre
    x_low = (gelu(h2_pre) + pos_ref[...]).astype(BF)
    x_ref[0] = x_low
    x_hat, _ = norm_stats(x_low.astype(F32))
    n1_ref[0] = (x_hat * vec_ref[2:3, :] + vec_ref[3:4, :]).astype(BF)


def front(mel, halo, pos, w1, w2, vec):
    n_batch, mel_len, n_mel = mel.shape
    frames, width = pos.shape
    rows = frames + 8
    per = lambda *shape: pl.BlockSpec((1,) + shape, lambda b: (b,) + (0,) * len(shape))
    whole = lambda a: pl.BlockSpec(a.shape, lambda b: (0,) * a.ndim)
    return pl.pallas_call(
        front_kernel, grid=(n_batch,),
        in_specs=[per(mel_len, n_mel), per(4, n_mel), whole(pos), whole(w1), whole(w2), whole(vec)],
        out_specs=[per(frames, 3 * width), per(frames, width), per(frames, width), per(frames, width)],
        out_shape=[jax.ShapeDtypeStruct((n_batch, frames, 3 * width), BF), jax.ShapeDtypeStruct((n_batch, frames, width), F32),
                   jax.ShapeDtypeStruct((n_batch, frames, width), BF), jax.ShapeDtypeStruct((n_batch, frames, width), BF)],
        scratch_shapes=[pltpu.VMEM((2 * rows + 8, LANES), F32), pltpu.VMEM((rows, width), F32), pltpu.VMEM((rows, width), F32)],
        cost_estimate=pl.CostEstimate(flops=8_000_000_000, bytes_accessed=8_000_000, transcendentals=0),
        name='front',
    )(mel, halo, pos, w1, w2, vec)


def project_kernel(g_ref, n1_ref, out_ref):
    heads, n_batch, rows3, frames = out_ref.shape
    width = n1_ref.shape[2]
    w_all = g_ref[:, 0:rows3, 0:width].reshape(heads * rows3, width)
    bias = g_ref[:, 0:rows3, width:width + 1].astype(F32).reshape(heads * rows3, 1)
    for b in range(n_batch):
        out_ref[:, b] = (mm_nt(w_all, n1_ref[b]) + bias).astype(BF).reshape(heads, rows3, frames)


def project(g, n1, rows3):
    heads = g.shape[0]
    n_batch, frames, _ = n1.shape
    return pl.pallas_call(
        project_kernel, out_shape=jax.ShapeDtypeStruct((heads, n_batch, rows3, frames), BF),
        in_specs=[pl.BlockSpec(memory_space=pltpu.VMEM)] * 2, out_specs=pl.BlockSpec(memory_space=pltpu.VMEM),
        cost_estimate=pl.CostEstimate(flops=2_000_000_000, bytes_accessed=4_000_000, transcendentals=0),
        name='project',
    )(g, n1)


def attend_kernel(qkv_ref, o_ref, p_ref, k_scr, v_scr, s_scr0, s_scr1):
    step = pl.program_id(1)
    parts, _, _, frames = qkv_ref.shape
    hd = HEAD_DIM

    @pl.when(step == 0)
    def _():
        for part in range(parts):
            k_scr[part * frames:(part + 1) * frames, :] = qkv_ref[part, 0, hd:2 * hd, :].astype(F32).T.astype(BF)
            v_scr[:, part * frames:(part + 1) * frames] = qkv_ref[part, 0, 2 * hd:3 * hd, :]

    factor = HEAD_DIM ** -0.5 * math.log2(math.e)
    scrs = (s_scr0, s_scr1)
    tops = []
    for sub in range(2):
        q_t = qkv_ref[step * 2 + sub, 0, 0:hd, :]
        top = None
        for part in range(parts):
            rows = slice(part * frames, (part + 1) * frames)
            s = mm(k_scr[rows, :], q_t)
            scrs[sub][rows, :] = s
            part_top = jnp.max(s.reshape(frames // 8, 8, frames), axis=0)
            top = part_top if top is None else jnp.maximum(top, part_top)
        tops.append(jnp.max(top, axis=0, keepdims=True))
    invs = []
    for sub in range(2):
        total = jnp.zeros((8, frames), F32)
        for part in range(parts):
            rows = slice(part * frames, (part + 1) * frames)
            e = jnp.exp2((scrs[sub][rows, :] - tops[sub]) * factor)
            scrs[sub][rows, :] = e
            total = total + jnp.sum(e.reshape(frames // 8, 8, frames), axis=0)
        invs.append(1.0 / jnp.sum(total, axis=0, keepdims=True))
    for sub in range(2):
        out = jnp.zeros((hd, frames), F32)
        for part in range(parts):
            rows = slice(part * frames, (part + 1) * frames)
            p = (scrs[sub][rows, :] * invs[sub]).astype(BF)
            p_ref[0, sub, rows, :] = p
            out = out + mm(v_scr[:, rows], p)
        o_ref[sub, 0] = out.astype(BF)


def attend(qkv):
    parts, n_batch, rows3, frames = qkv.shape
    total = parts * frames
    return pl.pallas_call(
        attend_kernel, grid=(n_batch, parts // 2),
        in_specs=[pl.BlockSpec((parts, 1, rows3, frames), lambda b, i: (0, b, 0, 0))],
        out_specs=[pl.BlockSpec((2, 1, HEAD_DIM, frames), lambda b, i: (i, b, 0, 0)),
                   pl.BlockSpec((1, 2, total, frames), lambda b, i: (b, i, 0, 0))],
        out_shape=[jax.ShapeDtypeStruct((parts, n_batch, HEAD_DIM, frames), BF),
                   jax.ShapeDtypeStruct((n_batch, parts, total, frames), BF)],
        scratch_shapes=[pltpu.VMEM((total, HEAD_DIM), BF), pltpu.VMEM((HEAD_DIM, total), BF),
                        pltpu.VMEM((total, frames), F32), pltpu.VMEM((total, frames), F32)],
        compiler_params=pltpu.CompilerParams(dimension_semantics=('arbitrary', 'arbitrary')),
        cost_estimate=pl.CostEstimate(flops=20_000_000_000, bytes_accessed=20_000_000, transcendentals=0),
        name='attend',
    )(qkv)


def attend_back_kernel(qkv_ref, do_ref, o_ref, p_ref, out_ref, dbias_ref, v_scr, kt_scr, dk_scr, dv_scr, dq_sum):
    b, step = pl.program_id(0), pl.program_id(1)
    parts, _, _, frames = qkv_ref.shape
    hd = HEAD_DIM

    @pl.when(step == 0)
    def _():
        for part in range(parts):
            rows = slice(part * frames, (part + 1) * frames)
            v_scr[rows, :] = qkv_ref[part, 0, 2 * hd:3 * hd, :].astype(F32).T.astype(BF)
            kt_scr[:, rows] = qkv_ref[part, 0, hd:2 * hd, :]
        dk_scr[...] = jnp.zeros_like(dk_scr)
        dv_scr[...] = jnp.zeros_like(dv_scr)

    @pl.when((step == 0) & (b == 0))
    def _():
        dq_sum[...] = jnp.zeros_like(dq_sum)
        dbias_ref[...] = jnp.zeros_like(dbias_ref)

    do_t = do_ref[step, 0]
    q = qkv_ref[step, 0, 0:hd, :].astype(F32).T.astype(BF)
    do = do_t.astype(F32).T.astype(BF)
    delta = colsum(do_t.astype(F32) * o_ref[step, 0].astype(F32))
    dq = jnp.zeros((hd, frames), F32)
    for part in range(parts):
        rows = slice(part * frames, (part + 1) * frames)
        p = p_ref[0, 0, rows, :]
        dp = mm(v_scr[rows, :], do_t)
        ds = (p.astype(F32) * (dp - delta)).astype(BF)
        dv_scr[rows, :] += mm(p, do)
        dk_scr[rows, :] += mm(ds, q)
        dq = dq + mm(kt_scr[:, rows], ds)
    dq = dq * (HEAD_DIM ** -0.5)
    out_ref[step, 0, 0:hd, :] = dq.astype(BF)
    dq_sum[...] += dq

    @pl.when(step == parts - 1)
    def _():
        for part in range(parts):
            rows = slice(part * frames, (part + 1) * frames)
            out_ref[part, 0, hd:2 * hd, :] = (dk_scr[rows, :] * (HEAD_DIM ** -0.5)).T.astype(BF)
            out_ref[part, 0, 2 * hd:3 * hd, :] = dv_scr[rows, :].T.astype(BF)
        dbias_ref[1:2, :] += colsum(dv_scr[...])
        dbias_ref[0:1, :] = colsum(dq_sum[...].T)


def attend_back(qkv, do, o, p):
    parts, n_batch, rows3, frames = qkv.shape
    total = parts * frames
    block = lambda rows: pl.BlockSpec((parts, 1, rows, frames), lambda b, i: (0, b, 0, 0))
    return pl.pallas_call(
        attend_back_kernel, grid=(n_batch, parts),
        in_specs=[block(rows3), block(HEAD_DIM), block(HEAD_DIM), pl.BlockSpec((1, 1, total, frames), lambda b, i: (b, i, 0, 0))],
        out_specs=[block(rows3), pl.BlockSpec((8, HEAD_DIM), lambda b, i: (0, 0))],
        out_shape=[jax.ShapeDtypeStruct(qkv.shape, BF), jax.ShapeDtypeStruct((8, HEAD_DIM), F32)],
        scratch_shapes=[pltpu.VMEM((total, HEAD_DIM), BF), pltpu.VMEM((HEAD_DIM, total), BF),
                        pltpu.VMEM((total, HEAD_DIM), F32), pltpu.VMEM((total, HEAD_DIM), F32), pltpu.VMEM((HEAD_DIM, frames), F32)],
        compiler_params=pltpu.CompilerParams(dimension_semantics=('arbitrary', 'arbitrary')),
        cost_estimate=pl.CostEstimate(flops=40_000_000_000, bytes_accessed=20_000_000, transcendentals=0),
        name='attend_back',
    )(qkv, do, o, p)


def mlp_kernel(o_ref, x_ref, dy_ref, wo_ref, w1_ref, w2_ref, vec_ref, y_ref, da_ref, dmid_ref, dwo_ref, dw1_ref, dw2_ref, dvec_ref,
               mid_scr, n2_scr, y_scr, dn_scr, hat_scr, rstd_scr):
    j = pl.program_id(0)
    heads, n_batch, hd, frames = o_ref.shape
    rows, width = x_ref.shape
    fc = w2_ref.shape[1]

    @pl.when(j == 0)
    def _():
        wo = wo_ref[:, :, 0:width].reshape(heads * hd, width)
        for b in range(n_batch):
            blk = slice(b * frames, (b + 1) * frames)
            attn = mm_tn(o_ref[:, b].reshape(heads * hd, frames), wo)
            mid = (x_ref[blk, :].astype(F32) + attn + vec_ref[4:5, :]).astype(BF)
            mid_scr[blk, :] = mid
            x_hat, rstd = norm_stats(mid.astype(F32))
            hat_scr[blk, :] = x_hat
            rstd_scr[blk, :] = jnp.broadcast_to(rstd, (frames, LANES))
            n2_scr[blk, :] = (x_hat * vec_ref[5:6, :] + vec_ref[6:7, :]).astype(BF)
        y_scr[...] = jnp.zeros_like(y_scr)
        dn_scr[...] = jnp.zeros_like(dn_scr)

    w1 = w1_ref[0, 0:width, :]
    pre = mm(n2_scr[...], w1) + w1_ref[0, width:width + 1, :].astype(F32)
    cdf = phi_cdf(pre)
    hidden = (pre * cdf).astype(BF)
    grad = cdf + pre * (jnp.exp(pre * pre * -0.5) * (1.0 / math.sqrt(2.0 * math.pi)))
    d_pre = mm_nt(dy_ref[...], w2_ref[0]) * grad
    d_low = d_pre.astype(BF)
    y_scr[...] += mm(hidden, w2_ref[0])
    dn_scr[...] += mm_nt(d_low, w1)
    dw2_ref[0] = mm_tn(hidden, dy_ref[...]).astype(BF)
    dw1_ref[0, 0:width, :] = mm_tn(n2_scr[...], d_low).astype(BF)
    dw1_ref[0, width:width + BIAS_ROWS, :] = jnp.broadcast_to(colsum(d_pre), (BIAS_ROWS, fc)).astype(BF)

    @pl.when(j == pl.num_programs(0) - 1)
    def _():
        wo = wo_ref[:, :, 0:width].reshape(heads * hd, width)
        y_ref[...] = (mid_scr[...].astype(F32) + y_scr[...] + vec_ref[7:8, :]).astype(BF)
        dvec_ref[...] = jnp.zeros_like(dvec_ref)
        d_wo = jnp.zeros((heads * hd, width), F32)
        for b in range(n_batch):
            blk = slice(b * frames, (b + 1) * frames)
            dy = dy_ref[blk, :].astype(F32)
            x_hat = hat_scr[blk, :]
            d_n2 = dn_scr[blk, :]
            d_mid = dy + norm_back(d_n2, x_hat, rstd_scr[blk, 0:1], vec_ref[5:6, :])
            dmid_ref[blk, :] = d_mid
            dvec_ref[0:1, :] += colsum(dy)
            dvec_ref[1:2, :] += colsum(d_n2 * x_hat)
            dvec_ref[2:3, :] += colsum(d_n2)
            dvec_ref[3:4, :] += colsum(d_mid)
            mid_low = d_mid.astype(BF)
            da_ref[:, b] = mm_nt(wo, mid_low).astype(BF).reshape(heads, hd, frames)
            d_wo = d_wo + mm(o_ref[:, b].reshape(heads * hd, frames), mid_low)
        dwo_ref[...] = d_wo.astype(BF).reshape(heads, hd, width)


def mlp(o, x, dy, g, w1, w2, vec):
    heads, n_batch, hd, frames = o.shape
    rows, width = x.shape
    chunks, fc, _ = w2.shape
    whole = lambda shape: pl.BlockSpec(shape, lambda j: (0,) * len(shape))
    chunk = lambda shape: pl.BlockSpec((1,) + shape[1:], lambda j: (j,) + (0,) * (len(shape) - 1))
    sds = jax.ShapeDtypeStruct
    outs = [sds((rows, width), BF), sds((heads, n_batch, hd, frames), BF), sds((rows, width), F32), sds((heads, hd, width), BF),
            sds(w1.shape, BF), sds(w2.shape, BF), sds((VEC_ROWS, width), F32)]
    return pl.pallas_call(
        mlp_kernel, grid=(chunks,),
        in_specs=[whole(o.shape), whole(x.shape), whole(dy.shape),
                  pl.BlockSpec((heads, hd, g.shape[2]), lambda j: (0, g.shape[1] // hd - 1, 0)),
                  chunk(w1.shape), chunk(w2.shape), whole(vec.shape)],
        out_specs=[whole(s.shape) for s in outs[:4]] + [chunk(w1.shape), chunk(w2.shape), whole(outs[6].shape)],
        out_shape=outs,
        scratch_shapes=[pltpu.VMEM((rows, width), BF), pltpu.VMEM((rows, width), BF), pltpu.VMEM((rows, width), F32),
                        pltpu.VMEM((rows, width), F32), pltpu.VMEM((rows, width), F32), pltpu.VMEM((rows, LANES), F32)],
        compiler_params=pltpu.CompilerParams(dimension_semantics=('arbitrary',)),
        cost_estimate=pl.CostEstimate(flops=14_000_000_000, bytes_accessed=12_000_000, transcendentals=0),
        name='mlp',
    )(o, x, dy, g, w1, w2, vec)


def embed_back_kernel(dqkv_ref, g_ref, n1_ref, x_ref, dmid_ref, h2_ref, h1_ref, dwo_ref, vec_ref, dh2_ref, dw_ref, dw2_ref, dvec_ref):
    heads, n_batch, rows3, frames = dqkv_ref.shape
    width = n1_ref.shape[2]
    w_all = g_ref[:, 0:rows3, 0:width].reshape(heads * rows3, width)
    dvec_ref[...] = jnp.zeros_like(dvec_ref)
    d_all = [dqkv_ref[:, b].reshape(heads * rows3, frames) for b in range(n_batch)]
    for b in range(n_batch):
        d_n1 = mm_tn(d_all[b], w_all)
        x_hat, rstd = norm_stats(x_ref[b].astype(F32))
        d_x = dmid_ref[b * frames:(b + 1) * frames, :] + norm_back(d_n1, x_hat, rstd, vec_ref[2:3, :])
        d_h2 = d_x * gelu_grad(h2_ref[b])
        dvec_ref[0:1, :] += colsum(d_n1 * x_hat)
        dvec_ref[1:2, :] += colsum(d_n1)
        dvec_ref[2:3, :] += colsum(d_h2)
        dh2_ref[b] = d_h2.astype(BF)
    d_w = mm(d_all[0], n1_ref[0])
    d_conv = mm_tn(h1_ref[0], dh2_ref[0])
    for b in range(1, n_batch):
        d_w = d_w + mm(d_all[b], n1_ref[b])
        d_conv = d_conv + mm_tn(h1_ref[b], dh2_ref[b])
    dw_ref[:, 0:rows3, :] = d_w.astype(BF).reshape(heads, rows3, width)
    dw_ref[:, rows3:, :] = dwo_ref[...]
    dw2_ref[...] = d_conv.astype(BF)


def embed_back(dqkv, g, n1, x, dmid, h2, h1, dwo, vec):
    n_batch, frames, width = n1.shape
    heads = dqkv.shape[0]
    sds = jax.ShapeDtypeStruct
    return pl.pallas_call(
        embed_back_kernel,
        in_specs=[pl.BlockSpec(memory_space=pltpu.VMEM)] * 9,
        out_specs=[pl.BlockSpec(memory_space=pltpu.VMEM)] * 4,
        out_shape=[sds((n_batch, frames, width), BF), sds((heads, g.shape[1], width), BF), sds((3 * width, width), BF),
                   sds((VEC_ROWS, width), F32)],
        cost_estimate=pl.CostEstimate(flops=8_000_000_000, bytes_accessed=8_000_000, transcendentals=0),
        name='embed_back',
    )(dqkv, g, n1, x, dmid, h2, h1, dwo, vec)


def stem_back_kernel(mel_ref, halo_ref, dh2_ref, edge_ref, w1_ref, w2_ref, vec_ref, dmel_ref, dw_ref, db_ref,
                     m_scr, d_scr, e_scr, o_scr, out_scr):
    rank = lax.axis_index('tp')
    first = pl.program_id(0) == 0
    n_mel = mel_ref.shape[2]
    frames, width = dh2_ref.shape[1:]
    rows = e_scr.shape[0]
    load_mel(m_scr, mel_ref, halo_ref)
    taps = mel_taps(m_scr, rows, n_mel)
    even, odd = conv_one(taps, w1_ref, vec_ref[0:1, :])
    d_scr[0:8, :] = jnp.zeros((8, width), F32)
    d_scr[frames:frames + 16, :] = jnp.zeros((16, width), F32)
    d_scr[1:frames + 1, :] = dh2_ref[0].astype(F32)
    edge = edge_ref[0].astype(F32)
    d_scr[0:1, :] = edge[0:1]
    d_scr[frames + 1:frames + 2, :] = edge[1:2]
    here = d_scr[0:rows, :].astype(BF)
    after = d_scr[1:rows + 1, :].astype(BF)
    ids = row_ids(rows, width)
    own = (ids >= 1) & (ids <= frames)
    d_even = jnp.where((ids >= 1) & (ids <= frames + 1), mm_nt(here, w2_ref[width:2 * width, :]) * gelu_grad(even), 0.0)
    lowest = jnp.where(rank == 0, 1, 0)
    d_odd = mm_nt(here, w2_ref[2 * width:3 * width, :]) + mm_nt(after, w2_ref[0:width, :])
    d_odd = jnp.where((ids >= lowest) & (ids <= frames), d_odd * gelu_grad(odd), 0.0)
    e_own = jnp.where(own, d_even, 0.0)
    o_own = jnp.where(own, d_odd, 0.0)
    d_bias = colsum(e_own) + colsum(o_own)
    e_own, o_own = e_own.astype(BF), o_own.astype(BF)
    d_w = [mm_tn(taps[t], e_own) + mm_tn(taps[t + 1], o_own) for t in range(3)]

    @pl.when(first)
    def _():
        db_ref[...] = jnp.zeros_like(db_ref)
        dw_ref[...] = jnp.zeros_like(dw_ref)

    db_ref[0:1, :] += d_bias
    for t in range(3):
        dw_ref[t] += d_w[t]
    e_scr[...] = d_even
    o_scr[...] = d_odd
    e_here = e_scr[1:frames + 1, :].astype(BF)
    e_after = e_scr[2:frames + 2, :].astype(BF)
    o_here = o_scr[1:frames + 1, :].astype(BF)
    o_before = o_scr[0:frames, :].astype(BF)
    out_scr[pl.ds(0, frames, stride=2), 0:n_mel] = (mm_nt(e_here, w1_ref[1]) + mm_nt(o_here, w1_ref[0]) + mm_nt(o_before, w1_ref[2]))
    out_scr[pl.ds(1, frames, stride=2), 0:n_mel] = (mm_nt(e_here, w1_ref[2]) + mm_nt(o_here, w1_ref[1]) + mm_nt(e_after, w1_ref[0]))
    dmel_ref[0] = out_scr[:, 0:n_mel].astype(BF)


def stem_back(mel, halo, dh2, edge, w1, w2, vec):
    n_batch, mel_len, n_mel = mel.shape
    frames, width = dh2.shape[1:]
    rows = frames + 8
    per = lambda *shape: pl.BlockSpec((1,) + shape, lambda b: (b,) + (0,) * len(shape))
    whole = lambda shape: pl.BlockSpec(shape, lambda b: (0,) * len(shape))
    sds = jax.ShapeDtypeStruct
    return pl.pallas_call(
        stem_back_kernel, grid=(n_batch,),
        in_specs=[per(mel_len, n_mel), per(4, n_mel), per(frames, width), per(2, width), whole(w1.shape), whole(w2.shape),
                  whole(vec.shape)],
        out_specs=[per(mel_len, n_mel), whole(w1.shape), whole((VEC_ROWS, width))],
        out_shape=[sds(mel.shape, BF), sds(w1.shape, F32), sds((VEC_ROWS, width), F32)],
        scratch_shapes=[pltpu.VMEM((2 * rows + 8, LANES), F32), pltpu.VMEM((frames + 16, width), F32),
                        pltpu.VMEM((rows, width), F32), pltpu.VMEM((rows, width), F32), pltpu.VMEM((mel_len, LANES), F32)],
        compiler_params=pltpu.CompilerParams(dimension_semantics=('arbitrary',)),
        cost_estimate=pl.CostEstimate(flops=8_000_000_000, bytes_accessed=8_000_000, transcendentals=0),
        name='stem_back',
    )(mel, halo, dh2, edge, w1, w2, vec)


def device_step(mel_in, pos_table, w_conv1, b_conv1, w_conv2, b_conv2, ln1_gain, ln1_bias, w_query, b_query,
                w_key, w_value, b_value, w_out, b_out, ln2_gain, ln2_bias, w_fc1, b_fc1, w_fc2, b_fc2, grad_y,
                group_size):
    n_batch, mel_len, n_mel = mel_in.shape
    frames, width = pos_table.shape
    fc = w_fc1.shape[1]
    hd = w_query.shape[1]
    rows3 = 3 * hd
    rows = n_batch * frames
    to_right = [(i, i + 1) for i in range(group_size - 1)]
    to_left = [(i + 1, i) for i in range(group_size - 1)]

    left = lax.ppermute(mel_in[:, -2:], 'tp', to_right)
    right = lax.ppermute(mel_in[:, :2], 'tp', to_left)
    halo = jnp.concatenate([left, right], axis=1)
    vec = jnp.stack([b_conv1, b_conv2, ln1_gain, ln1_bias, b_out, ln2_gain, ln2_bias, b_fc2]).astype(F32)
    w2_flat = w_conv2.reshape(3 * width, width)

    heads_w = jnp.concatenate([jnp.concatenate([w_query, w_key, w_value], axis=1).T, w_out], axis=0)
    heads_b = jnp.concatenate([b_query, jnp.zeros_like(b_query), b_value, jnp.zeros_like(b_query)])
    gathered = lax.all_gather(jnp.concatenate([heads_w, jnp.broadcast_to(heads_b[:, None], (4 * hd, LANES))], axis=1), 'tp')
    fc1_all = lax.all_gather(jnp.concatenate([w_fc1, jnp.broadcast_to(b_fc1[None], (BIAS_ROWS, fc))], axis=0), 'tp')
    fc2_all = lax.all_gather(w_fc2, 'tp')

    h1, h2_pre, x_embed, norm_one = front(mel_in, halo, pos_table, w_conv1, w2_flat, vec)
    qkv = exchange(project(gathered, norm_one, rows3), group_size, 0)
    o_heads, probs = attend(qkv)
    o_all = exchange(o_heads, group_size, 1)
    y_out, d_attn, d_mid, d_wo, d_fc1, d_fc2, vec_mlp = mlp(
        o_all, x_embed.reshape(rows, width), grad_y.reshape(rows, width), gathered, fc1_all, fc2_all, vec)
    fc1_own = lax.psum_scatter(d_fc1, 'tp', scatter_dimension=0).astype(F32)
    fc2_own = lax.psum_scatter(d_fc2, 'tp', scatter_dimension=0).astype(F32)
    d_o = exchange(d_attn, group_size, 2)
    d_heads, d_bias = attend_back(qkv, d_o, o_heads, probs)
    d_qkv = exchange(d_heads, group_size, 3)
    d_h2, d_w, d_conv2, vec_embed = embed_back(d_qkv, gathered, norm_one, x_embed, d_mid, h2_pre, h1, d_wo, vec)
    edge = jnp.stack([lax.ppermute(d_h2[:, -1], 'tp', to_right), lax.ppermute(d_h2[:, 0], 'tp', to_left)], axis=1)
    heads_own = lax.psum_scatter(d_w, 'tp', scatter_dimension=0).astype(F32)
    conv2_part = lax.psum_scatter(d_conv2.reshape(group_size, -1, width), 'tp', scatter_dimension=0)
    d_conv2_all = lax.all_gather(conv2_part, 'tp').astype(F32).reshape(w_conv2.shape)
    d_mel, d_conv1, vec_stem = stem_back(mel_in, halo, d_h2, edge, w_conv1, w2_flat, vec)
    small = jnp.concatenate([d_conv1.reshape(3 * n_mel, width), vec_mlp[0:4], vec_embed[0:3], vec_stem[0:1],
                             jnp.zeros((8, width), F32)]).astype(BF)
    small = all_sum(small.reshape(group_size, -1, width), group_size, 4).reshape(-1, width)
    d_conv1_all = small[:3 * n_mel].reshape(w_conv1.shape)
    vecs = small[3 * n_mel:]
    return (y_out.reshape(grad_y.shape), d_mel, d_conv1_all, vecs[7], d_conv2_all, vecs[6], vecs[4], vecs[5],
            heads_own[0:hd].T, d_bias[0], heads_own[hd:2 * hd].T, heads_own[2 * hd:3 * hd].T, d_bias[1],
            heads_own[3 * hd:], vecs[3], vecs[1], vecs[2], fc1_own[:width], fc1_own[width], fc2_own, vecs[0])


def solution(mesh):
    group_size = mesh.shape['tp']
    in_specs = (P('dp', 'tp', None), P('tp', None), P(), P(), P(), P(), P(), P(),
                P(None, 'tp'), P('tp'), P(None, 'tp'), P(None, 'tp'), P('tp'), P('tp', None), P(), P(), P(),
                P(None, 'tp'), P('tp'), P('tp', None), P(), P('dp', 'tp', None))
    out_specs = (P('dp', 'tp', None), P('dp', 'tp', None), P('dp', None, None), P('dp'), P('dp', None, None),
                 P('dp'), P('dp'), P('dp'), P('dp', 'tp'), P(('dp', 'tp')), P('dp', 'tp'), P('dp', 'tp'),
                 P(('dp', 'tp')), P(('dp', 'tp'), None), P('dp'), P('dp'), P('dp'), P('dp', 'tp'),
                 P(('dp', 'tp')), P(('dp', 'tp'), None), P('dp'))
    local_step = functools.partial(device_step, group_size=group_size)
    return jax.shard_map(local_step, mesh=mesh, in_specs=in_specs, out_specs=out_specs, check_vma=False)
```

```python
import functools
import math
import jax
import jax.numpy as jnp
from jax import lax
from jax.experimental import pallas as pl
from jax.experimental.pallas import tpu as pltpu
from jax.sharding import PartitionSpec as P

HEAD_DIM = 64
LN_EPS = 1e-5
BF = jnp.bfloat16
F32 = jnp.float32
LANES = 128
BIAS_ROWS = 16
VEC_ROWS = 8


def dims(lhs, rhs, contract_lhs, contract_rhs):
    return lax.dot_general(lhs, rhs, (((contract_lhs,), (contract_rhs,)), ((), ())), preferred_element_type=F32)


def mm(lhs, rhs):
    return dims(lhs, rhs, 1, 0)


def mm_nt(lhs, rhs):
    return dims(lhs, rhs, 1, 1)


def mm_tn(lhs, rhs):
    return dims(lhs, rhs, 0, 0)


def phi_cdf(x):
    return 0.5 * (1.0 + lax.erf(x * (0.5 ** 0.5)))


def gelu(x):
    return x * phi_cdf(x)


def gelu_grad(x):
    return phi_cdf(x) + x * (jnp.exp(x * x * -0.5) * (1.0 / math.sqrt(2.0 * math.pi)))


def norm_stats(x):
    centred = x - jnp.mean(x, axis=-1, keepdims=True)
    rstd = lax.rsqrt(jnp.mean(centred * centred, axis=-1, keepdims=True) + LN_EPS)
    return centred * rstd, rstd


def norm_back(d_out, x_hat, rstd, gain):
    a = d_out * gain
    return rstd * (a - jnp.mean(a, axis=-1, keepdims=True) - x_hat * jnp.mean(a * x_hat, axis=-1, keepdims=True))


def colsum(x):
    return jnp.sum(x, axis=0, keepdims=True)


def peer(index):
    return {'tp': index}


def entry_barrier(size, me):
    barrier = pltpu.get_barrier_semaphore()
    for step in range(1, size):
        pl.semaphore_signal(barrier, inc=1, device_id=peer(lax.rem(me + step, size)), device_id_type=pl.DeviceIdType.MESH)
    pl.semaphore_wait(barrier, size - 1)


def sibling(me):
    return me + 1 - 2 * lax.rem(me, 2)


def remote(src, dst, send_sem, recv_sem, to):
    return pltpu.make_async_remote_copy(src_ref=src, dst_ref=dst, send_sem=send_sem, recv_sem=recv_sem, device_id=peer(to),
                                        device_id_type=pl.DeviceIdType.MESH)


class Gather:
    def __init__(self, me, size, src, dst, send_sem, recv_sem):
        half = size // 2
        sib = sibling(me)
        self.first = [remote(src, dst.at[me], send_sem.at[0], recv_sem.at[0], sib)]
        self.relay = []
        for k in range(1, half):
            self.first.append(remote(src, dst.at[me], send_sem.at[k], recv_sem.at[k], lax.rem(me + 2 * k, size)))
            origin = lax.rem(me + size - 2 * k, size)
            self.relay.append(remote(dst.at[origin], dst.at[origin], send_sem.at[half + k], recv_sem.at[half + k], sib))

    def start(self):
        for copy in self.first[1:] + self.first[:1]:
            copy.start()

    def forward(self):
        for copy, onward in zip(self.first[1:], self.relay):
            copy.wait_recv()
            onward.start()

    def finish(self):
        self.first[0].wait()
        for copy in self.first[1:]:
            copy.wait_send()
        for onward in self.relay:
            onward.wait()


class Scatter:
    def __init__(self, me, size, x, own, near, far, sems, local_sem=None, part=None):
        self.half = size // 2
        self.own, self.near, self.far, self.x, self.me, self.size = own, near, far, x, me, size
        sib = sibling(me)
        send_a, recv_a, send_b, recv_b = sems
        self.stage_a = [remote(x.at[lax.rem(sib + 2 * k, size)], near.at[k], send_a.at[k], recv_a.at[k], sib)
                        for k in range(self.half)]
        self.loads = None if local_sem is None else [
            pltpu.make_async_copy(x.at[lax.rem(me + 2 * k, size)], own.at[k], local_sem.at[k]) for k in range(self.half)]
        parts = part or [(0, own.shape[1])]
        self.stage_b = [[remote(own.at[k, lo:hi], far.at[k, lo:hi], send_b.at[i, k], recv_b.at[i, k], lax.rem(me + 2 * k, size))
                         for k in range(1, self.half)] for i, (lo, hi) in enumerate(parts)]
        self.parts = parts

    def start(self):
        for copy in self.stage_a:
            copy.start()
        for load in self.loads or []:
            load.start()

    def middle(self):
        for k in range(self.half):
            if self.loads is None:
                self.own[k] = self.x[lax.rem(self.me + 2 * k, self.size)]
            else:
                self.loads[k].wait()
            self.stage_a[k].wait()
        for k in range(1, self.half):
            self.own[k] = (self.own[k].astype(F32) + self.near[k].astype(F32)).astype(BF)
        for copies in self.stage_b:
            for copy in copies:
                copy.start()

    def finish(self, i=0):
        lo, hi = self.parts[i]
        for copy in self.stage_b[i]:
            copy.wait()
        total = self.own[0, lo:hi].astype(F32) + self.near[0, lo:hi].astype(F32)
        for k in range(1, self.half):
            total = total + self.far[k, lo:hi].astype(F32)
        return total


def scatter_scratch(size, shape, parts=1):
    half = size // 2
    return [pltpu.VMEM((half,) + shape, BF)] * 3 + [pltpu.SemaphoreType.DMA((half,))] * 2 + [pltpu.SemaphoreType.DMA((parts, half))] * 2


VM = pl.BlockSpec(memory_space=pltpu.VMEM)
ANY = pl.BlockSpec(memory_space=pl.ANY)


def load_mel(m_scr, mel, halo, b):
    mel_len, n_mel = mel.shape
    total = m_scr.shape[0]
    m_scr[0:8, :] = jnp.zeros((8, m_scr.shape[1]), F32)
    m_scr[8 + mel_len:total, :] = jnp.zeros((total - 8 - mel_len, m_scr.shape[1]), F32)
    m_scr[8:8 + mel_len, 0:n_mel] = mel.astype(F32)
    m_scr[6:8, :] = halo[0, 2 * b:2 * b + 2, :]
    m_scr[8 + mel_len:10 + mel_len, :] = halo[1, 2 * b:2 * b + 2, :]


def mel_taps(m_scr, rows, n_mel):
    return [m_scr[pl.ds(5 + tap, rows, stride=2), :].astype(BF)[:, 0:n_mel] for tap in range(4)]


def conv_one(taps, w_ref, bias):
    even = mm(taps[0], w_ref[0]) + mm(taps[1], w_ref[1]) + mm(taps[2], w_ref[2]) + bias
    odd = mm(taps[1], w_ref[0]) + mm(taps[2], w_ref[1]) + mm(taps[3], w_ref[2]) + bias
    return even, odd


def row_ids(rows, width):
    return lax.broadcasted_iota(jnp.int32, (rows, width), 0)


def ring_edges(me, size, edge_ref, edge_scr, sems):
    right = remote(edge_ref.at[0], edge_scr.at[0], sems.at[0], sems.at[2], lax.rem(me + 1, size))
    left = remote(edge_ref.at[1], edge_scr.at[1], sems.at[1], sems.at[3], lax.rem(me + size - 1, size))
    return right, left


def masked_edges(me, size, edge_scr):
    side = lax.broadcasted_iota(jnp.int32, edge_scr.shape, 0)
    outside = ((side == 0) & (me == 0)) | ((side == 1) & (me == size - 1))
    return jnp.where(outside, 0.0, edge_scr[...])


def stem_kernel(size, mel_ref, edge_ref, pos_ref, w1_ref, w2_ref, vec_ref, heads_ref, h1_ref, h2_ref, x_ref, n1_ref, qkv_ref, g_ref,
                halo_ref, m_scr, e_scr, o_scr, edge_scr, edge_sem, send_sem, recv_sem):
    me = lax.axis_index('tp')
    n_batch, _, n_mel = mel_ref.shape
    frames, width = pos_ref.shape
    rows = e_scr.shape[0]
    rows3 = qkv_ref.shape[2]
    entry_barrier(size, me)
    edges = ring_edges(me, size, edge_ref, edge_scr, edge_sem)
    for copy in edges:
        copy.start()
    gather = Gather(me, size, heads_ref, g_ref, send_sem, recv_sem)
    gather.start()
    g_ref[me] = heads_ref[...]
    for copy in edges:
        copy.wait()
    halo_ref[...] = masked_edges(me, size, edge_scr)
    for b in range(n_batch):
        load_mel(m_scr, mel_ref[b], halo_ref, b)
        even, odd = conv_one(mel_taps(m_scr, rows, n_mel), w1_ref, vec_ref[0:1, :])
        e_scr[...] = gelu(even)
        o_scr[...] = gelu(odd)

        @pl.when(me == 0)
        def _():
            o_scr[0:1, :] = jnp.zeros((1, width), F32)

        h1_ref[b, :, 0:width] = o_scr[0:frames, :].astype(BF)
        h1_ref[b, :, width:2 * width] = e_scr[1:frames + 1, :].astype(BF)
        h1_ref[b, :, 2 * width:3 * width] = o_scr[1:frames + 1, :].astype(BF)
        h2_pre = mm(h1_ref[b], w2_ref[...]) + vec_ref[1:2, :]
        h2_ref[b] = h2_pre
        x_low = (gelu(h2_pre) + pos_ref[...]).astype(BF)
        x_ref[b] = x_low
        x_hat, _ = norm_stats(x_low.astype(F32))
        n1_ref[b] = (x_hat * vec_ref[2:3, :] + vec_ref[3:4, :]).astype(BF)
    gather.forward()
    gather.finish()
    w_all = g_ref[:, 0:rows3, :].reshape(size * rows3, width)
    ones = jnp.ones((BIAS_ROWS, frames), BF)
    bias = jnp.concatenate([mm_tn(g_ref[h, rows3:rows3 + BIAS_ROWS, 0:rows3], ones) for h in range(size)], axis=0)
    for b in range(n_batch):
        qkv_ref[:, b] = (mm_nt(w_all, n1_ref[b]) + bias).astype(BF).reshape(size, rows3, frames)


def stem(size, mel, edges, pos, w1, w2, vec, heads):
    n_batch, mel_len, n_mel = mel.shape
    frames, width = pos.shape
    rows = frames + 8
    rows3 = heads.shape[0] - BIAS_ROWS
    sds = jax.ShapeDtypeStruct
    return pl.pallas_call(
        functools.partial(stem_kernel, size),
        in_specs=[VM] * 7, out_specs=[VM] * 7,
        out_shape=[sds((n_batch, frames, 3 * width), BF), sds((n_batch, frames, width), F32), sds((n_batch, frames, width), BF),
                   sds((n_batch, frames, width), BF), sds((size, n_batch, rows3, frames), BF), sds((size,) + heads.shape, BF),
                   sds(edges.shape, F32)],
        scratch_shapes=[pltpu.VMEM((2 * rows + 8, LANES), F32), pltpu.VMEM((rows, width), F32), pltpu.VMEM((rows, width), F32),
                        pltpu.VMEM(edges.shape, F32), pltpu.SemaphoreType.DMA((4,)), pltpu.SemaphoreType.DMA((size,)),
                        pltpu.SemaphoreType.DMA((size,))],
        compiler_params=pltpu.CompilerParams(collective_id=0, has_side_effects=True),
        name='stem',
    )(mel, edges, pos, w1, w2, vec, heads)


def attend_kernel(size, qkv_in, w1_ref, w2_ref, o_all, o_own, p_hbm, qkv_ref, w1_all, w2_all, k_scr, v_scr, s_scr0, s_scr1, p_buf,
                  q_send, q_recv, o_send, o_recv, p_sem, w1_send, w1_recv, w2_send, w2_recv, own_sem):
    me = lax.axis_index('tp')
    parts, n_batch, rows3, frames = qkv_ref.shape
    hd = HEAD_DIM
    pairs = parts // 2
    factor = HEAD_DIM ** -0.5 * math.log2(math.e)
    scrs = (s_scr0, s_scr1)
    entry_barrier(size, me)
    arrivals = []
    for b in range(n_batch):
        arrivals.append([remote(qkv_in.at[lax.rem(me + k, size), b], qkv_ref.at[me, b], q_send.at[b, k], q_recv.at[b, k],
                                lax.rem(me + k, size)) for k in range(1, size)])
        for copy in arrivals[b]:
            copy.start()
        qkv_ref[me, b] = qkv_in[me, b]
    gathers = [Gather(me, size, w1_ref, w1_all, w1_send, w1_recv), Gather(me, size, w2_ref, w2_all, w2_send, w2_recv)]
    own = [pltpu.make_async_copy(w1_ref, w1_all.at[me], own_sem.at[0]), pltpu.make_async_copy(w2_ref, w2_all.at[me], own_sem.at[1])]
    for copy in own:
        copy.start()

    def p_copy(b, i):
        return pltpu.make_async_copy(p_buf.at[lax.rem(i, 2)], p_hbm.at[b, :, pl.ds(pl.multiple_of(i * 2 * frames, 2 * frames), 2 * frames)],
                                     p_sem.at[lax.rem(i, 2)])

    def send_out(b, i):
        for sub in range(2):
            to = 2 * i + sub

            @pl.when(to != me)
            def _():
                remote(o_own.at[to, b], o_all.at[me, b], o_send.at[b, to], o_recv.at[b, me], to).start()

            @pl.when(to == me)
            def _():
                o_all[me, b] = o_own[me, b]

    for b in range(n_batch):
        for copy in arrivals[b]:
            copy.wait()
        for part in range(parts):
            k_scr[part * frames:(part + 1) * frames, :] = qkv_ref[part, b, hd:2 * hd, :].astype(F32).T.astype(BF)
            v_scr[:, part * frames:(part + 1) * frames] = qkv_ref[part, b, 2 * hd:3 * hd, :]

        def body(i, carry):
            @pl.when(i >= 1)
            def _():
                send_out(b, i - 1)

            if b == 0:
                @pl.when(i == 1)
                def _():
                    gathers[0].start()
                    gathers[1].start()

                @pl.when(i >= 2)
                def _():
                    p_copy(b, i).wait()
            else:
                p_copy(b, i).wait()
            tops = []
            for sub in range(2):
                q_t = qkv_ref[2 * i + sub, b, 0:hd, :]
                top = None
                for part in range(parts):
                    rows = slice(part * frames, (part + 1) * frames)
                    s = mm(k_scr[rows, :], q_t)
                    scrs[sub][rows, :] = s
                    part_top = jnp.max(s.reshape(frames // 8, 8, frames), axis=0)
                    top = part_top if top is None else jnp.maximum(top, part_top)
                tops.append(jnp.max(top, axis=0, keepdims=True))
            invs = []
            for sub in range(2):
                total = jnp.zeros((8, frames), F32)
                for part in range(parts):
                    rows = slice(part * frames, (part + 1) * frames)
                    e = jnp.exp2((scrs[sub][rows, :] - tops[sub]) * factor)
                    scrs[sub][rows, :] = e
                    total = total + jnp.sum(e.reshape(frames // 8, 8, frames), axis=0)
                invs.append(1.0 / jnp.sum(total, axis=0, keepdims=True))
            for sub in range(2):
                out = jnp.zeros((hd, frames), F32)
                for part in range(parts):
                    rows = slice(part * frames, (part + 1) * frames)
                    p = (scrs[sub][rows, :] * invs[sub]).astype(BF)
                    p_buf[lax.rem(i, 2), rows, sub * frames:(sub + 1) * frames] = p
                    out = out + mm(v_scr[:, rows], p)
                o_own[2 * i + sub, b] = out.astype(BF)
            p_copy(b, i).start()
            return carry

        lax.fori_loop(0, pairs, body, 0)
        if b == n_batch - 1:
            for i in (pairs - 2, pairs - 1):
                p_copy(b, i).wait()
        send_out(b, pairs - 1)
    for gather in gathers:
        gather.forward()
    for b in range(n_batch):
        for k in range(1, size):
            to = lax.rem(me + k, size)
            remote(o_own.at[to, b], o_all.at[to, b], o_send.at[b, to], o_recv.at[b, to], to).wait()
    for gather in gathers:
        gather.finish()
    for copy in own:
        copy.wait()


def attend(size, qkv, w1, w2):
    parts, n_batch, rows3, frames = qkv.shape
    total = parts * frames
    sds = jax.ShapeDtypeStruct
    dma = pltpu.SemaphoreType.DMA
    return pl.pallas_call(
        functools.partial(attend_kernel, size),
        in_specs=[VM] * 3, out_specs=[VM, VM, ANY, VM, ANY, ANY],
        out_shape=[sds((parts, n_batch, HEAD_DIM, frames), BF), sds((parts, n_batch, HEAD_DIM, frames), BF),
                   sds((n_batch, total, total), BF), sds(qkv.shape, BF), sds((size,) + w1.shape, BF), sds((size,) + w2.shape, BF)],
        scratch_shapes=[pltpu.VMEM((total, HEAD_DIM), BF), pltpu.VMEM((HEAD_DIM, total), BF),
                        pltpu.VMEM((total, frames), F32), pltpu.VMEM((total, frames), F32), pltpu.VMEM((2, total, 2 * frames), BF),
                        dma((n_batch, size)), dma((n_batch, size)), dma((n_batch, size)), dma((n_batch, size)), dma((2,)),
                        dma((size,)), dma((size,)), dma((size,)), dma((size,)), dma((2,))],
        compiler_params=pltpu.CompilerParams(collective_id=1, has_side_effects=True),
        name='attend',
    )(qkv, w1, w2)


def attend_back_kernel(size, qkv_ref, da_ref, o_ref, p_hbm, dw1_hbm, dw2_hbm, out_all, dbias_ref, fc1_ref, fc2_ref,
                       do_scr, snd, dot_scr, do_all, q_all, delta_scr, ds_scr, p_buf, dq_scr, dv_sum,
                       a_send, a_recv, kv_send, kv_recv, dq_send, dq_recv, p_sem, load_sem,
                       own1, near1, far1, sa1, ra1, sb1, rb1, own2, near2, far2, sa2, ra2, sb2, rb2):
    me = lax.axis_index('tp')
    parts, n_batch, rows3, frames = qkv_ref.shape
    hd = HEAD_DIM
    scale = HEAD_DIM ** -0.5
    total = parts * frames
    entry_barrier(size, me)
    arrivals = []
    for b in range(n_batch):
        arrivals.append([remote(da_ref.at[lax.rem(me + k, size), b], do_scr.at[me, b], a_send.at[b, k], a_recv.at[b, k],
                                lax.rem(me + k, size)) for k in range(1, size)])
        for copy in arrivals[b]:
            copy.start()
        do_scr[me, b] = da_ref[me, b]
    scat1 = Scatter(me, size, dw1_hbm, own1, near1, far1, (sa1, ra1, sb1, rb1), load_sem.at[0])
    scat2 = Scatter(me, size, dw2_hbm, own2, near2, far2, (sa2, ra2, sb2, rb2), load_sem.at[1])
    scat1.start()
    scat2.start()

    def p_copy(b, i):
        return pltpu.make_async_copy(p_hbm.at[b, pl.ds(pl.multiple_of(i * frames, frames), frames), :], p_buf.at[lax.rem(i, 2)],
                                     p_sem.at[lax.rem(i, 2)])

    def send_piece(to, b, lo, hi, send_sem, recv_sem):
        @pl.when(to != me)
        def _():
            remote(snd.at[to, b, lo:hi], out_all.at[me, b, lo:hi], send_sem.at[b, to], recv_sem.at[b, me], to).start()

        @pl.when(to == me)
        def _():
            out_all[me, b, lo:hi, :] = snd[me, b, lo:hi, :]

    dbias_ref[...] = jnp.zeros_like(dbias_ref)
    dv_sum[...] = jnp.zeros_like(dv_sum)
    dq_rows = jnp.zeros((hd, frames), F32)
    for b in range(n_batch):
        p_copy(b, 0).start()
        for copy in arrivals[b]:
            copy.wait()
        if b == 0:
            scat1.middle()
        else:
            scat2.middle()
        for part in range(parts):
            rows = slice(part * frames, (part + 1) * frames)
            do_t = do_scr[part, b]
            dot_scr[:, rows] = do_t
            do_all[rows, :] = do_t.astype(F32).T.astype(BF)
            q_all[rows, :] = qkv_ref[part, b, 0:hd, :].astype(F32).T.astype(BF)
            delta_scr[0:1, rows] = colsum(do_t.astype(F32) * o_ref[part, b].astype(F32))
        dq_scr[...] = jnp.zeros_like(dq_scr)

        def body(i, carry):
            slot = lax.rem(i, 2)
            p_copy(b, i).wait()

            @pl.when(i + 1 < parts)
            def _():
                p_copy(b, i + 1).start()

            @pl.when(i >= 1)
            def _():
                send_piece(i - 1, b, hd, 3 * hd, kv_send, kv_recv)

            v = qkv_ref[i, b, 2 * hd:3 * hd, :].astype(F32).T.astype(BF)
            k_t = qkv_ref[i, b, hd:2 * hd, :]
            for c in range(parts // 2):
                cols = slice(c * 2 * frames, (c + 1) * 2 * frames)
                dp = mm(v, dot_scr[:, cols])
                ds = (p_buf[slot, :, cols].astype(F32) * (dp - delta_scr[0:1, cols])).astype(BF)
                ds_scr[:, cols] = ds
                dq_scr[:, cols] += mm(k_t, ds)
            dv = mm(p_buf[slot], do_all[...])
            dk = mm(ds_scr[...], q_all[...]) * scale
            dv_sum[...] += dv
            snd[i, b, hd:2 * hd, :] = dk.T.astype(BF)
            snd[i, b, 2 * hd:3 * hd, :] = dv.T.astype(BF)
            return carry

        lax.fori_loop(0, parts, body, 0)
        for part in range(parts):
            dq = dq_scr[:, part * frames:(part + 1) * frames] * scale
            dq_rows = dq_rows + dq
            snd[part, b, 0:hd, :] = dq.astype(BF)
        send_piece(parts - 1, b, hd, 3 * hd, kv_send, kv_recv)
        for part in range(parts):
            send_piece(part, b, 0, hd, dq_send, dq_recv)
    dbias_ref[0:1, :] = colsum(dq_rows.T)
    dbias_ref[1:2, :] = colsum(dv_sum[...])
    fc1_ref[...] = scat1.finish()
    fc2_ref[...] = scat2.finish()
    for b in range(n_batch):
        for k in range(1, size):
            to = lax.rem(me + k, size)
            remote(snd.at[to, b, hd:3 * hd], out_all.at[to, b, hd:3 * hd], kv_send.at[b, to], kv_recv.at[b, to], to).wait()
            remote(snd.at[to, b, 0:hd], out_all.at[to, b, 0:hd], dq_send.at[b, to], dq_recv.at[b, to], to).wait()


def attend_back(size, qkv, da, o, p, dw1, dw2):
    parts, n_batch, rows3, frames = qkv.shape
    total = parts * frames
    sds = jax.ShapeDtypeStruct
    dma = pltpu.SemaphoreType.DMA
    return pl.pallas_call(
        functools.partial(attend_back_kernel, size),
        in_specs=[VM, VM, VM, ANY, ANY, ANY], out_specs=[VM] * 4,
        out_shape=[sds(qkv.shape, BF), sds((8, HEAD_DIM), F32), sds(dw1.shape[1:], F32), sds(dw2.shape[1:], F32)],
        scratch_shapes=[pltpu.VMEM(da.shape, BF), pltpu.VMEM(qkv.shape, BF), pltpu.VMEM((HEAD_DIM, total), BF),
                        pltpu.VMEM((total, HEAD_DIM), BF), pltpu.VMEM((total, HEAD_DIM), BF), pltpu.VMEM((8, total), F32),
                        pltpu.VMEM((frames, total), BF), pltpu.VMEM((2, frames, total), BF), pltpu.VMEM((HEAD_DIM, total), F32),
                        pltpu.VMEM((frames, HEAD_DIM), F32)]
        + [dma((n_batch, size))] * 6 + [dma((2,)), dma((2, size // 2))]
        + scatter_scratch(size, dw1.shape[1:]) + scatter_scratch(size, dw2.shape[1:]),
        compiler_params=pltpu.CompilerParams(collective_id=2, has_side_effects=True),
        name='attend_back',
    )(qkv, da, o, p, dw1, dw2)


def mlp_kernel(o_ref, x_ref, dy_ref, wo_ref, w1_ref, w2_ref, vec_ref, y_ref, da_ref, dmid_ref, dwo_ref, dw1_ref, dw2_ref, dvec_ref,
               mid_scr, n2_scr, y_scr, dn_scr, hat_scr, rstd_scr):
    j = pl.program_id(0)
    heads, n_batch, hd, frames = o_ref.shape
    rows, width = x_ref.shape
    fc = dw2_ref.shape[1]
    w2 = w2_ref[0]

    @pl.when(j == 0)
    def _():
        wo = wo_ref[...].reshape(heads * hd, width)
        for b in range(n_batch):
            blk = slice(b * frames, (b + 1) * frames)
            attn = mm_tn(o_ref[:, b].reshape(heads * hd, frames), wo)
            mid = (x_ref[blk, :].astype(F32) + attn + vec_ref[4:5, :]).astype(BF)
            mid_scr[blk, :] = mid
            x_hat, rstd = norm_stats(mid.astype(F32))
            hat_scr[blk, :] = x_hat
            rstd_scr[blk, :] = jnp.broadcast_to(rstd, (frames, LANES))
            n2_scr[blk, :] = (x_hat * vec_ref[5:6, :] + vec_ref[6:7, :]).astype(BF)
        y_scr[...] = jnp.zeros_like(y_scr)
        dn_scr[...] = jnp.zeros_like(dn_scr)

    w1 = w1_ref[0, 0:width, :]
    pre = mm(n2_scr[...], w1) + w1_ref[0, width:width + 1, :].astype(F32)
    cdf = phi_cdf(pre)
    hidden = (pre * cdf).astype(BF)
    grad = cdf + pre * (jnp.exp(pre * pre * -0.5) * (1.0 / math.sqrt(2.0 * math.pi)))
    d_pre = mm_nt(dy_ref[...], w2) * grad
    d_low = d_pre.astype(BF)
    y_scr[...] += mm(hidden, w2)
    dn_scr[...] += mm_nt(d_low, w1)
    dw2_ref[0] = mm_tn(hidden, dy_ref[...]).astype(BF)
    dw1_ref[0, 0:width, :] = mm_tn(n2_scr[...], d_low).astype(BF)
    dw1_ref[0, width:width + BIAS_ROWS, :] = jnp.broadcast_to(colsum(d_pre), (BIAS_ROWS, fc)).astype(BF)

    @pl.when(j == pl.num_programs(0) - 1)
    def _():
        wo = wo_ref[...].reshape(heads * hd, width)
        y_ref[...] = (mid_scr[...].astype(F32) + y_scr[...] + vec_ref[7:8, :]).astype(BF)
        dvec_ref[...] = jnp.zeros_like(dvec_ref)
        d_wo = jnp.zeros((heads * hd, width), F32)
        for b in range(n_batch):
            blk = slice(b * frames, (b + 1) * frames)
            dy = dy_ref[blk, :].astype(F32)
            x_hat = hat_scr[blk, :]
            d_n2 = dn_scr[blk, :]
            d_mid = dy + norm_back(d_n2, x_hat, rstd_scr[blk, 0:1], vec_ref[5:6, :])
            dmid_ref[blk, :] = d_mid
            dvec_ref[0:1, :] += colsum(dy)
            dvec_ref[1:2, :] += colsum(d_n2 * x_hat)
            dvec_ref[2:3, :] += colsum(d_n2)
            dvec_ref[3:4, :] += colsum(d_mid)
            mid_low = d_mid.astype(BF)
            da_ref[:, b] = mm_nt(wo, mid_low).astype(BF).reshape(heads, hd, frames)
            d_wo = d_wo + mm(o_ref[:, b].reshape(heads * hd, frames), mid_low)
        dwo_ref[...] = d_wo.astype(BF).reshape(heads, hd, width)


def mlp(o, x, dy, w1, w2, vec):
    heads, n_batch, hd, frames = o.shape
    rows, width = x.shape
    chunks, fc = w2.shape[0], w2.shape[1] - hd
    whole = lambda shape: pl.BlockSpec(shape, lambda j: (0,) * len(shape))
    chunk = lambda shape: pl.BlockSpec((1,) + shape[1:], lambda j: (j,) + (0,) * (len(shape) - 1))
    sds = jax.ShapeDtypeStruct
    outs = [sds((rows, width), BF), sds((heads, n_batch, hd, frames), BF), sds((rows, width), F32), sds((heads, hd, width), BF),
            sds(w1.shape, BF), sds((chunks, fc, width), BF), sds((VEC_ROWS, width), F32)]
    return pl.pallas_call(
        mlp_kernel, grid=(chunks,),
        in_specs=[whole(o.shape), whole(x.shape), whole(dy.shape),
                  pl.BlockSpec((heads, hd, width), lambda j: (0, fc // hd, 0)),
                  chunk(w1.shape), chunk((chunks, fc, width)), whole(vec.shape)],
        out_specs=[whole(s.shape) for s in outs[:4]] + [chunk(w1.shape), chunk((chunks, fc, width)), whole(outs[6].shape)],
        out_shape=outs,
        scratch_shapes=[pltpu.VMEM((rows, width), BF), pltpu.VMEM((rows, width), BF), pltpu.VMEM((rows, width), F32),
                        pltpu.VMEM((rows, width), F32), pltpu.VMEM((rows, width), F32), pltpu.VMEM((rows, LANES), F32)],
        compiler_params=pltpu.CompilerParams(dimension_semantics=('arbitrary',)),
        cost_estimate=pl.CostEstimate(flops=14_000_000_000, bytes_accessed=12_000_000, transcendentals=0),
        name='mlp',
    )(o, x, dy, w2, w1, w2, vec)


def embed_back_kernel(dqkv_ref, g_ref, n1_ref, x_ref, dmid_ref, h2_ref, h1_ref, dwo_ref, vec_ref, dh2_ref, dw_ref, edge_ref, dvec_ref):
    heads, n_batch, rows3, frames = dqkv_ref.shape
    width = n1_ref.shape[2]
    w_all = g_ref[:, 0:rows3, 0:width].reshape(heads * rows3, width)
    dvec_ref[...] = jnp.zeros_like(dvec_ref)
    edge_ref[...] = jnp.zeros_like(edge_ref)
    d_all = [dqkv_ref[:, b].reshape(heads * rows3, frames) for b in range(n_batch)]
    for b in range(n_batch):
        d_n1 = mm_tn(d_all[b], w_all)
        x_hat, rstd = norm_stats(x_ref[b].astype(F32))
        d_x = dmid_ref[b * frames:(b + 1) * frames, :] + norm_back(d_n1, x_hat, rstd, vec_ref[2:3, :])
        d_h2 = d_x * gelu_grad(h2_ref[b])
        dvec_ref[0:1, :] += colsum(d_n1 * x_hat)
        dvec_ref[1:2, :] += colsum(d_n1)
        dvec_ref[2:3, :] += colsum(d_h2)
        dh2_ref[b] = d_h2.astype(BF)
        edge_ref[0, b:b + 1, :] = d_h2[frames - 1:frames].astype(BF).astype(F32)
        edge_ref[1, b:b + 1, :] = d_h2[0:1].astype(BF).astype(F32)
    d_w = mm(d_all[0], n1_ref[0])
    d_conv = mm_tn(h1_ref[0], dh2_ref[0])
    for b in range(1, n_batch):
        d_w = d_w + mm(d_all[b], n1_ref[b])
        d_conv = d_conv + mm_tn(h1_ref[b], dh2_ref[b])
    dw_ref[:, 0:rows3, :] = d_w.astype(BF).reshape(heads, rows3, width)
    dw_ref[:, rows3:rows3 + HEAD_DIM, :] = dwo_ref[...]
    dw_ref[:, rows3 + HEAD_DIM:, :] = d_conv.astype(BF).reshape(heads, 3 * width // heads, width)


def embed_back(dqkv, g, n1, x, dmid, h2, h1, dwo, vec):
    n_batch, frames, width = n1.shape
    heads = dqkv.shape[0]
    sds = jax.ShapeDtypeStruct
    return pl.pallas_call(
        embed_back_kernel,
        in_specs=[pl.BlockSpec(memory_space=pltpu.VMEM)] * 9,
        out_specs=[pl.BlockSpec(memory_space=pltpu.VMEM)] * 4,
        out_shape=[sds((n_batch, frames, width), BF), sds((heads, dqkv.shape[2] + HEAD_DIM + 3 * width // heads, width), BF), sds((2, 8, width), F32),
                   sds((VEC_ROWS, width), F32)],
        cost_estimate=pl.CostEstimate(flops=8_000_000_000, bytes_accessed=8_000_000, transcendentals=0),
        name='embed_back',
    )(dqkv, g, n1, x, dmid, h2, h1, dwo, vec)


def tail_kernel(size, mel_ref, halo_ref, dh2_ref, edge_ref, w1_ref, w2_ref, vec_ref, grads_hbm, vmlp_ref, vemb_ref,
                dmel_ref, heads_ref, conv_ref, small_ref,
                m_scr, d_scr, e_scr, o_scr, out_scr, edge_scr, sum_scr, small_scr, mine, whole, edge_sem, load_sem, g_send, g_recv,
                own1, near1, far1, sa1, ra1, sb1, rb1, own2, near2, far2, sa2, ra2, sb2, rb2):
    me = lax.axis_index('tp')
    n_batch, _, n_mel = mel_ref.shape
    frames, width = dh2_ref.shape[1:]
    rows = e_scr.shape[0]
    head_rows = heads_ref.shape[0]
    all_rows = grads_hbm.shape[1]
    conv_rows = all_rows - head_rows
    entry_barrier(size, me)
    edges = ring_edges(me, size, edge_ref, edge_scr, edge_sem)
    for copy in edges:
        copy.start()
    scat = Scatter(me, size, grads_hbm, own1, near1, far1, (sa1, ra1, sb1, rb1), load_sem,
                   part=[(head_rows, all_rows), (0, head_rows)])
    scat.start()
    small = Scatter(me, size, small_scr, own2, near2, far2, (sa2, ra2, sb2, rb2))
    for copy in edges:
        copy.wait()
    edge_scr[...] = masked_edges(me, size, edge_scr)
    sum_scr[...] = jnp.zeros_like(sum_scr)
    ids = row_ids(rows, width)
    lowest = jnp.where(me == 0, 1, 0)
    for b in range(n_batch):
        load_mel(m_scr, mel_ref[b], halo_ref, b)
        taps = mel_taps(m_scr, rows, n_mel)
        even, odd = conv_one(taps, w1_ref, vec_ref[0:1, :])
        d_scr[0:8, :] = jnp.zeros((8, width), F32)
        d_scr[frames:frames + 16, :] = jnp.zeros((16, width), F32)
        d_scr[1:frames + 1, :] = dh2_ref[b].astype(F32)
        d_scr[0:1, :] = edge_scr[0, b:b + 1, :]
        d_scr[frames + 1:frames + 2, :] = edge_scr[1, b:b + 1, :]
        here = d_scr[0:rows, :].astype(BF)
        after = d_scr[1:rows + 1, :].astype(BF)
        own = (ids >= 1) & (ids <= frames)
        d_even = jnp.where((ids >= 1) & (ids <= frames + 1), mm_nt(here, w2_ref[width:2 * width, :]) * gelu_grad(even), 0.0)
        d_odd = mm_nt(here, w2_ref[2 * width:3 * width, :]) + mm_nt(after, w2_ref[0:width, :])
        d_odd = jnp.where((ids >= lowest) & (ids <= frames), d_odd * gelu_grad(odd), 0.0)
        e_own = jnp.where(own, d_even, 0.0)
        o_own = jnp.where(own, d_odd, 0.0)
        sum_scr[3 * n_mel + 7:3 * n_mel + 8, :] += colsum(e_own) + colsum(o_own)
        e_own, o_own = e_own.astype(BF), o_own.astype(BF)
        for t in range(3):
            sum_scr[t * n_mel:(t + 1) * n_mel, :] += mm_tn(taps[t], e_own) + mm_tn(taps[t + 1], o_own)
        e_scr[...] = d_even
        o_scr[...] = d_odd
        e_here = e_scr[1:frames + 1, :].astype(BF)
        e_after = e_scr[2:frames + 2, :].astype(BF)
        o_here = o_scr[1:frames + 1, :].astype(BF)
        o_before = o_scr[0:frames, :].astype(BF)
        out_scr[pl.ds(0, frames, stride=2), 0:n_mel] = mm_nt(e_here, w1_ref[1]) + mm_nt(o_here, w1_ref[0]) + mm_nt(o_before, w1_ref[2])
        out_scr[pl.ds(1, frames, stride=2), 0:n_mel] = mm_nt(e_here, w1_ref[2]) + mm_nt(o_here, w1_ref[1]) + mm_nt(e_after, w1_ref[0])
        dmel_ref[b] = out_scr[:, 0:n_mel].astype(BF)
        if b == 0:
            scat.middle()
    sum_scr[3 * n_mel:3 * n_mel + 4, :] = vmlp_ref[0:4, :]
    sum_scr[3 * n_mel + 4:3 * n_mel + 7, :] = vemb_ref[0:3, :]
    small_scr[...] = sum_scr[...].astype(BF).reshape(small_scr.shape)
    small.start()
    small.middle()
    mine[0:conv_rows, :] = scat.finish(0).astype(BF)
    mine[conv_rows:, :] = small.finish().astype(BF)
    gather = Gather(me, size, mine, whole, g_send, g_recv)
    gather.start()
    heads_ref[...] = scat.finish(1)
    gather.forward()
    gather.finish()
    whole[me] = mine[...]
    conv_ref[...] = whole[:, 0:conv_rows, :].astype(F32)
    small_ref[...] = whole[:, conv_rows:, :].astype(F32)


def tail(size, mel, halo, dh2, edge, w1, w2, vec, grads, vmlp, vemb):
    n_batch, mel_len, n_mel = mel.shape
    frames, width = dh2.shape[1:]
    rows = frames + 8
    head_rows = 4 * HEAD_DIM
    conv_rows = grads.shape[1] - head_rows
    small_rows = -(-(3 * n_mel + 8) // (16 * size)) * 16
    half = size // 2
    sds = jax.ShapeDtypeStruct
    dma = pltpu.SemaphoreType.DMA
    return pl.pallas_call(
        functools.partial(tail_kernel, size),
        in_specs=[VM] * 7 + [ANY, VM, VM], out_specs=[VM] * 4,
        out_shape=[sds(mel.shape, BF), sds((head_rows, width), F32), sds((size, conv_rows, width), F32), sds((size, small_rows, width), F32)],
        scratch_shapes=[pltpu.VMEM((2 * rows + 8, LANES), F32), pltpu.VMEM((frames + 16, width), F32),
                        pltpu.VMEM((rows, width), F32), pltpu.VMEM((rows, width), F32), pltpu.VMEM((mel_len, LANES), F32),
                        pltpu.VMEM(edge.shape, F32), pltpu.VMEM((size * small_rows, width), F32),
                        pltpu.VMEM((size, small_rows, width), BF), pltpu.VMEM((conv_rows + small_rows, width), BF),
                        pltpu.VMEM((size, conv_rows + small_rows, width), BF), dma((4,)), dma((half,)), dma((size,)), dma((size,))]
        + scatter_scratch(size, grads.shape[1:], 2) + scatter_scratch(size, (small_rows, width)),
        compiler_params=pltpu.CompilerParams(collective_id=3, has_side_effects=True),
        name='tail',
    )(mel, halo, dh2, edge, w1, w2, vec, grads, vmlp, vemb)


def device_step(mel_in, pos_table, w_conv1, b_conv1, w_conv2, b_conv2, ln1_gain, ln1_bias, w_query, b_query,
                w_key, w_value, b_value, w_out, b_out, ln2_gain, ln2_bias, w_fc1, b_fc1, w_fc2, b_fc2, grad_y,
                group_size):
    n_batch, mel_len, n_mel = mel_in.shape
    frames, width = pos_table.shape
    fc = w_fc1.shape[1]
    hd = w_query.shape[1]
    rows3 = 3 * hd
    rows = n_batch * frames
    edges = jnp.stack([mel_in[:, -2:], mel_in[:, :2]]).astype(F32).reshape(2, 2 * n_batch, n_mel)
    edges = jnp.pad(edges, ((0, 0), (0, 8 - 2 * n_batch), (0, LANES - n_mel)))
    vec = jnp.stack([b_conv1, b_conv2, ln1_gain, ln1_bias, b_out, ln2_gain, ln2_bias, b_fc2]).astype(F32)
    w2_flat = w_conv2.reshape(3 * width, width)
    bias = jnp.concatenate([b_query, jnp.zeros_like(b_query), b_value])
    bias = jnp.pad(bias[None], ((0, BIAS_ROWS - 1), (0, width - rows3)))
    heads_w = jnp.concatenate([jnp.concatenate([w_query, w_key, w_value], axis=1).T, bias], axis=0)
    fc1_w = jnp.concatenate([w_fc1, jnp.broadcast_to(b_fc1[None], (BIAS_ROWS, fc))], axis=0)
    fc2_w = jnp.concatenate([w_fc2, w_out], axis=0)

    h1, h2_pre, x_embed, norm_one, qkv_send, heads_all, halo = stem(group_size, mel_in, edges, pos_table, w_conv1, w2_flat, vec, heads_w)
    o_all, o_heads, probs, qkv, fc1_all, fc2_all = attend(group_size, qkv_send, fc1_w, fc2_w)
    y_out, d_attn, d_mid, d_wo, d_fc1, d_fc2, vec_mlp = mlp(
        o_all, x_embed.reshape(rows, width), grad_y.reshape(rows, width), fc1_all, fc2_all, vec)
    d_qkv, d_bias, fc1_own, fc2_own = attend_back(group_size, qkv, d_attn, o_heads, probs, d_fc1, d_fc2)
    d_h2, d_w, d_edge, vec_embed = embed_back(d_qkv, heads_all, norm_one, x_embed, d_mid, h2_pre, h1, d_wo, vec)
    d_mel, heads_own, d_conv2, small = tail(group_size, mel_in, halo, d_h2, d_edge, w_conv1, w2_flat, vec, d_w, vec_mlp, vec_embed)
    small = small.reshape(-1, width)
    d_conv1 = small[:3 * n_mel].reshape(w_conv1.shape)
    vecs = small[3 * n_mel:]
    return (y_out.reshape(grad_y.shape), d_mel, d_conv1, vecs[7], d_conv2.reshape(w_conv2.shape), vecs[6], vecs[4], vecs[5],
            heads_own[0:hd].T, d_bias[0], heads_own[hd:2 * hd].T, heads_own[2 * hd:3 * hd].T, d_bias[1],
            heads_own[3 * hd:], vecs[3], vecs[1], vecs[2], fc1_own[:width], fc1_own[width], fc2_own, vecs[0])


def solution(mesh):
    group_size = mesh.shape['tp']
    in_specs = (P('dp', 'tp', None), P('tp', None), P(), P(), P(), P(), P(), P(),
                P(None, 'tp'), P('tp'), P(None, 'tp'), P(None, 'tp'), P('tp'), P('tp', None), P(), P(), P(),
                P(None, 'tp'), P('tp'), P('tp', None), P(), P('dp', 'tp', None))
    out_specs = (P('dp', 'tp', None), P('dp', 'tp', None), P('dp', None, None), P('dp'), P('dp', None, None),
                 P('dp'), P('dp'), P('dp'), P('dp', 'tp'), P(('dp', 'tp')), P('dp', 'tp'), P('dp', 'tp'),
                 P(('dp', 'tp')), P(('dp', 'tp'), None), P('dp'), P('dp'), P('dp'), P('dp', 'tp'),
                 P(('dp', 'tp')), P(('dp', 'tp'), None), P('dp'))
    local_step = functools.partial(device_step, group_size=group_size)
    return jax.shard_map(local_step, mesh=mesh, in_specs=in_specs, out_specs=out_specs, check_vma=False)
```
